512 devices in a mesh: seq: 64 (over z, x, core), head: 8 (over y).
Axes of the slice: x: 4, y: 8, z: 8, core: 2. Of those that a mesh axis runs over, the one named last changes fastest.
Arguments:
- query_rows: bfloat16 [32768, 64, 128], P('seq', 'head'), may hold values from -6 to 6
- key_rows: bfloat16 [32768, 64, 128], P('seq', 'head'), may hold values from -6 to 6
- value_rows: bfloat16 [32768, 64, 128], P('seq', 'head'), may hold values from -6 to 6
- log_decay: float32 [32768, 64], P('seq', 'head'), may hold values from -1.5 to 0, as said below
- state_in: float32 [128, 64, 128], P(None, 'head'), may hold values from -768 to 768
- decode_query: bfloat16 [8, 64, 128], P(None, 'head'), may hold values from -6 to 6
- decode_key: bfloat16 [8, 64, 128], P(None, 'head'), may hold values from -6 to 6
- decode_value: bfloat16 [8, 64, 128], P(None, 'head'), may hold values from -6 to 6
- decode_decay: float32 [8, 64], P(None, 'head'), may hold values from -0.5 to -0.02
Outputs:
- attended: bfloat16 [32768, 64, 128], P('seq', 'head')
- final_state: float32 [128, 64, 128], P('seq', 'head')
- decode_out: float32 [8, 64, 128], P(None, 'head')
The draws below stay inside these ranges and needn't reach their ends.
Inputs may be any that keep to these rules, and one draw needn't show every extreme that they name: log_decay is never positive.
All inputs are finite; a program needn't handle non-finite values.
Results may differ from the reference program's by a relative error of at most 0.0035.
Values sent between devices are 32-bit elements; how exact they have to be, the bound alone decides.
A program may use at most 64 MiB of HBM per device.

```python
import jax
import jax.numpy as jnp
from jax import lax

HEAD_COUNT = 64
DH = 128
TOK_DEV = 512
GROUP = 512
DECODE = 8
WINDOW_TOKENS = 32768


def draw_log_decay(key, part):
    sequence_lanes = jax.random.split(key, 7)
    fast_cut = 5
    fast_heads = jax.random.randint(sequence_lanes[0], (HEAD_COUNT,), 0, 10) < fast_cut
    slow_total = jax.random.uniform(sequence_lanes[1], (HEAD_COUNT,), jnp.float32, 0.1, 0.5)
    fast_rate = jax.random.uniform(sequence_lanes[2], (HEAD_COUNT,), jnp.float32, 1.0 / 50.0, 1.0 / 30.0)
    baseline_decay_rate = jnp.where(fast_heads, fast_rate, slow_total / WINDOW_TOKENS)
    split_divisor = jax.random.uniform(sequence_lanes[3], (WINDOW_TOKENS // TOK_DEV, HEAD_COUNT), jnp.float32, 0.7, 1.4)
    split_divisor = jnp.repeat(split_divisor, TOK_DEV, axis=0)
    jitter_level = jax.random.uniform(sequence_lanes[4], (WINDOW_TOKENS, HEAD_COUNT), jnp.float32, 0.5, 1.5)
    spike_start_index = jax.random.randint(sequence_lanes[5], (2, HEAD_COUNT), 0, WINDOW_TOKENS)
    spike_length = jax.random.uniform(sequence_lanes[6], (2, HEAD_COUNT), jnp.float32, 0.22, 0.69)
    token_positions = jnp.arange(WINDOW_TOKENS)[:, None]
    decay_spikes = jnp.where(token_positions == spike_start_index[0][None, :], spike_length[0][None, :], 0.0)
    decay_spikes = decay_spikes + jnp.where(token_positions == spike_start_index[1][None, :], spike_length[1][None, :], 0.0)
    return -(baseline_decay_rate[None, :] * split_divisor * jitter_level + decay_spikes)


def level_of(own_key, dims, cuts, least, largest):
    def one(dim, parts):
        draws = jax.random.uniform(jax.random.fold_in(jax.random.fold_in(own_key, 6), dim), (parts,), jnp.float32, least / len(cuts), largest / len(cuts))
        return jnp.repeat(jnp.exp(draws), dims[dim] // parts).reshape((-1,) + (1,) * (len(dims) - dim - 1))

    gain = one(*cuts[0])
    for cut in cuts[1:]:
        gain = gain * one(*cut)
    return gain


def scatter_about(rng, dims, spread, most, shards=(), held_as=jnp.bfloat16):
    result = spread * jax.random.normal(rng, dims, jnp.float32)
    if shards:
        result = result * level_of(rng, dims, shards, -0.22, 0.18)
    return jnp.clip(result, -most, most).astype(held_as)


def setup_inputs(seed: int = 0) -> dict:
    key_of = jax.random.split(jax.random.key(seed), 10)
    return {
        "query_rows": scatter_about(key_of[0], (WINDOW_TOKENS, HEAD_COUNT, DH), 1.0, 6.0, ((0, 64), (1, 8))),
        "key_rows": scatter_about(key_of[1], (WINDOW_TOKENS, HEAD_COUNT, DH), 1.0, 6.0, ((0, 64), (1, 8))),
        "value_rows": scatter_about(key_of[2], (WINDOW_TOKENS, HEAD_COUNT, DH), 1.0, 6.0, ((0, 64), (1, 8))),
        "log_decay": draw_log_decay(jax.random.fold_in(key_of[9], 71), 0),
        "state_in": scatter_about(key_of[4], (DH, HEAD_COUNT, DH), 128.0, 768.0, ((1, 8),), jnp.float32),
        "decode_query": scatter_about(key_of[5], (DECODE, HEAD_COUNT, DH), 1.0, 6.0, ((1, 8),)),
        "decode_key": scatter_about(key_of[6], (DECODE, HEAD_COUNT, DH), 1.0, 6.0, ((1, 8),)),
        "decode_value": scatter_about(key_of[7], (DECODE, HEAD_COUNT, DH), 1.0, 6.0, ((1, 8),)),
        "decode_decay": jnp.clip(-0.5 + 0.48 * jax.random.uniform(key_of[8], (DECODE, HEAD_COUNT), jnp.float32) ** level_of(key_of[8], (DECODE, HEAD_COUNT), ((1, 8),), -0.2, 0.2), -0.5, -0.02),
    }


norm_eps = 1e-06

def normalize(mixed):
    return mixed * lax.rsqrt(lax.optimization_barrier(jnp.mean(mixed * mixed, axis=-1, keepdims=True)) + norm_eps)

def block_step(carried, pieces):
    queries, keys_blk, values_blk, decays = pieces
    cumulative = jnp.cumsum(decays, axis=0)
    transposed = cumulative.T
    token_positions = jnp.arange(GROUP)
    causal_mask = token_positions[:, None] >= token_positions[None, :]
    gaps = transposed[:, :, None] - transposed[:, None, :]
    factors = jnp.exp(jnp.where(causal_mask[None], gaps, -jnp.inf))
    query_wide = queries.astype(jnp.float32)
    key_wide = keys_blk.astype(jnp.float32)
    value_wide = values_blk.astype(jnp.float32)
    scores = jnp.einsum('ihd,jhd->hij', query_wide, key_wide, precision=lax.Precision.HIGHEST)
    masked = (scores * factors).astype(jnp.bfloat16).astype(jnp.float32)
    intra = jnp.einsum('hij,jhd->ihd', masked, value_wide, precision=lax.Precision.HIGHEST)
    inter = jnp.exp(cumulative)[:, :, None] * jnp.einsum('ihd,dhe->ihe', query_wide, carried, precision=lax.Precision.HIGHEST)
    attended = normalize(intra + inter).astype(jnp.bfloat16)
    last = cumulative[-1]
    weighted = key_wide * jnp.exp(last[None, :] - cumulative)[:, :, None]
    updated = jnp.exp(last)[None, :, None] * carried + jnp.einsum('jhd,jhe->dhe', weighted, value_wide, precision=lax.Precision.HIGHEST)
    return (updated, attended)

def reference(query_rows, key_rows, value_rows, log_decay, state_in, decode_query, decode_key, decode_value, decode_decay):
    blocks = WINDOW_TOKENS // GROUP
    shaped = (query_rows.reshape(blocks, GROUP, HEAD_COUNT, DH), key_rows.reshape(blocks, GROUP, HEAD_COUNT, DH), value_rows.reshape(blocks, GROUP, HEAD_COUNT, DH), log_decay.reshape(blocks, GROUP, HEAD_COUNT))
    final_state, outputs = lax.scan(block_step, state_in.astype(jnp.float32), shaped)
    attended = outputs.reshape(WINDOW_TOKENS, HEAD_COUNT, DH)
    running = final_state
    readings = []
    for step in range(DECODE):
        key_now = decode_key[step].astype(jnp.float32)
        value_now = decode_value[step].astype(jnp.float32)
        running = jnp.exp(decode_decay[step])[None, :, None] * running + key_now.T[:, :, None] * value_now[None, :, :]
        query_now = decode_query[step].astype(jnp.float32)
        readings.append(jnp.einsum('hd,dhe->he', query_now, running, precision=lax.Precision.HIGHEST))
    decode_out = normalize(jnp.stack(readings, axis=0))
    return (attended, final_state, decode_out)
```

```python
import functools

import jax
import jax.numpy as jnp
from jax import lax
from jax.experimental import pallas as pl
from jax.experimental.pallas import tpu as pltpu
from jax.sharding import Mesh
from jax.sharding import PartitionSpec as P

GROUP = 512
DECODE = 8
DH = 128
HEADS = 8
X, C = 4, 2
SEQ = ("seq_0", "seq_1", "seq_2")
MESH = pl.DeviceIdType.MESH
F32, BF16 = jnp.float32, jnp.bfloat16
norm_eps = 1e-06

HALF = 256
QUARTER = 64
DECAY = HALF
EXTRA = HALF + 8
CORE_ROWS = HALF + 8 + 32
X_ROWS = QUARTER + 16

FILL = ((0, 2), (2, 5), (5, 8))


def halves(wide):
    high = wide.astype(BF16)
    return high, (wide - high.astype(F32)).astype(BF16)


def dot(a, b):
    return jnp.dot(a, b, preferred_element_type=F32)


def dot_nt(a, b):
    return lax.dot_general(a, b, (((1,), (1,)), ((), ())), preferred_element_type=F32)


def scaled(tile, rows):
    count = rows.shape[0]
    return (rows.reshape(count // 8, 8, DH) * tile[None]).reshape(count, DH)


def kernel(
    Z,
    q_hbm, k_hbm, v_hbm, ld_hbm, si_hbm, dq_hbm, dk_hbm, dv_hbm, dd_hbm,
    out_hbm, fs_ref, dec_ref,
    kb, vb, qb, kf, vf, qf, ldb, si, dqb, dkb, dvb, ddb, dqf, dkf, dvf,
    perm_s, cum_s, w_s, kT, vh, qp, ecol, intra, ob,
    bbuf, cbuf, tbuf, xbuf, rbuf, zbuf, zs, zr, xs, pc, ps, pp,
    sitile, rin, dint, dexp,
    in_sem, out_sem,
    core_s, core_r, x_s, x_r, z_s, z_r, zr_s, zr_r, xr_s, xr_r, cr_s, cr_r,
):
    ZR = QUARTER // Z
    R = ZR // 4
    zi, xi, ci = (lax.axis_index(a) for a in SEQ)
    first = ci == 0

    half = GROUP // 2
    copies = {}

    def fetch(name, src, dst, slot):
        copies[name] = pltpu.make_async_copy(src, dst, in_sem.at[slot])
        copies[name].start()

    fetch("ld", ld_hbm, ldb, 0)
    for i in range(2):
        rows = pl.ds(i * half, half)
        fetch(f"k{i}", k_hbm.at[rows], kb.at[rows], 1 + i)
    for i in range(2):
        rows = pl.ds(i * half, half)
        fetch(f"v{i}", v_hbm.at[rows], vb.at[rows], 3 + i)
    fetch("dq", dq_hbm, dqb, 5)
    fetch("q", q_hbm, qb, 6)
    fetch("dk", dk_hbm, dkb, 7)
    fetch("dv", dv_hbm, dvb, 8)
    fetch("dd", dd_hbm, ddb, 9)
    fetch("si", si_hbm, si, 10)

    barrier = pltpu.get_barrier_semaphore()
    partners = [{"seq_2": 1 - ci}]
    partners += [{"seq_1": lax.rem(xi + i, X)} for i in range(1, X)]
    partners += [{"seq_0": lax.rem(zi + i, Z)} for i in range(1, Z)]
    for partner in partners:
        pl.semaphore_signal(barrier, inc=1, device_id=partner, device_id_type=MESH)

    at = lax.broadcasted_iota(jnp.int32, (DH, DH), 0)
    feature = lax.broadcasted_iota(jnp.int32, (DH, DH), 1)
    r_at = at & (R - 1)
    z_at = (at // R) & (Z - 1)
    x_at = (at // (R * Z)) & (X - 1)
    c_at = at // (R * Z * X)
    owner_feature = ((z_at * X + x_at) * C + c_at) * R + r_at
    perm_s[...] = jnp.where(owner_feature == feature, 1.0, 0.0).astype(BF16)

    upper = jnp.where(at <= feature, 1.0, 0.0).astype(BF16)
    copies["ld"].wait()
    quarters = jnp.concatenate([ldb[:, i * DH : (i + 1) * DH] for i in range(4)], axis=0)
    p1, rest = quarters.astype(BF16), None
    rest = quarters - p1.astype(F32)
    p2 = rest.astype(BF16)
    p3 = (rest - p2.astype(F32)).astype(BF16)
    part = dot(p1, upper) + dot(p2, upper) + dot(p3, upper)
    before = jnp.zeros((HEADS, 1), F32)
    for i in range(4):
        piece = part[i * HEADS : (i + 1) * HEADS]
        cum_s[:, i * DH : (i + 1) * DH] = piece + before
        before = before + piece[:, DH - 1 : DH]
    w_s[...] = jnp.exp(before - cum_s[...])
    decay = jnp.broadcast_to(jnp.exp(before), (HEADS, DH))
    for g in range(2):
        for c in range(C):
            for i in range(2):
                bbuf[g, c, DECAY + 4 * i : DECAY + 4 * i + 4, :] = decay[4 * g : 4 * g + 4]

    def spread(src, dst, start):
        @pl.loop(0, 4)
        def _(i):
            rows = src[pl.ds(start + i * 64, 64)].astype(F32)
            dst[pl.ds((start + i * 64) * HEADS, 64 * HEADS), :] = rows.reshape(64 * HEADS, DH)

    for i in range(2):
        copies[f"k{i}"].wait()
        spread(kb, kf, i * half)
    for i in range(2):
        copies[f"v{i}"].wait()
        spread(vb, vf, i * half)
    copies["dq"].wait()
    dqf[...] = dqb[...].astype(F32).reshape(DECODE * HEADS, DH)

    pending = []

    def send(src, dst, send_sem, recv_sem, where):
        copy = pltpu.make_async_remote_copy(
            src_ref=src, dst_ref=dst, send_sem=send_sem, recv_sem=recv_sem,
            device_id=where, device_id_type=MESH,
        )
        copy.start()
        pending.append(copy)
        return copy

    perm = perm_s[...]
    no_rows = jnp.zeros((8, DH), F32)
    core_copy, x_copy, z_copy, zr_copy, xr_copy, cr_copy = ({} for _ in range(6))
    for g in range(2):
        for j in range(4):
            h = 4 * g + j
            k_h = kf[pl.ds(h, GROUP, stride=HEADS), :].astype(BF16)
            v_h = vf[pl.ds(h, GROUP, stride=HEADS), :].astype(BF16)
            vh[h] = v_h
            dq_h = dqf[pl.ds(h, DECODE, stride=HEADS), :]
            left = jnp.concatenate([perm, jnp.concatenate([dq_h, no_rows], axis=0).astype(BF16)], axis=0)
            k_t = dot_nt(left, k_h)
            kT[h] = k_t[:DH].astype(BF16)
            high, low = halves(k_t * w_s[h : h + 1, :])
            state = dot(high, v_h) + dot(low, v_h)
            for c in range(C):
                bbuf.at[g, c][pl.ds(j, DH // 2, stride=4), :] = state[c * 64 : c * 64 + 64]
            bbuf.at[1, g][pl.ds(EXTRA + j, DECODE, stride=4), :] = state[DH : DH + DECODE]
        if g == 0:
            pl.semaphore_wait(barrier, len(partners))
        rows = pl.ds(0, CORE_ROWS if g else EXTRA)
        core_copy[g] = send(
            bbuf.at[g, 1 - ci, rows], cbuf.at[g, rows], core_s.at[g], core_r.at[g], {"seq_2": 1 - ci}
        )

    def core_weights(g):
        own, other = bbuf[g, ci, DECAY : DECAY + 8, :], cbuf[g, DECAY : DECAY + 8, :]
        return jnp.where(first, other, 1.0), jnp.where(first, 1.0, own), own * other

    for g in range(2):
        core_copy[g].wait_recv()
        w_own, w_other, both = core_weights(g)
        for i in range(X):
            rows = slice(i * QUARTER, (i + 1) * QUARTER)
            tbuf[g, i, 0:QUARTER, :] = scaled(w_own, bbuf[g, ci, rows, :]) + scaled(w_other, cbuf[g, rows, :])
            tbuf[g, i, QUARTER : QUARTER + 8, :] = both
        if g:
            w_own, w_other, _ = core_weights(ci)
            for i in range(X):
                rows = slice(EXTRA + 8 * i, EXTRA + 8 * i + 8)
                tbuf[g, i, QUARTER + 8 : X_ROWS, :] = w_own * bbuf[g, ci, rows, :] + w_other * cbuf[g, rows, :]
        rows = pl.ds(0, X_ROWS if g else QUARTER + 8)
        for i in range(1, X):
            there = lax.rem(xi + i, X)
            x_copy[g, i] = send(
                tbuf.at[g, there, rows], xbuf.at[g, xi, rows], x_s.at[g, i], x_r.at[g, i], {"seq_1": there}
            )
        xbuf[g, xi, rows, :] = tbuf[g, xi, rows, :]

    causal = lax.broadcasted_iota(jnp.int32, (DH, DH), 0) >= lax.broadcasted_iota(jnp.int32, (DH, DH), 1)

    def block_attention(start, stop):
        @pl.loop(start, stop)
        def _(h):
            q_h = qf[pl.ds(h, GROUP, stride=HEADS), :].astype(BF16)
            qp[h] = dot_nt(q_h, perm_s[...]).astype(BF16)
            row = cum_s[pl.ds(h, 1), :]
            column = jnp.broadcast_to(row, (DH, GROUP)).T
            ecol[h] = jnp.exp(column)
            for i in range(4):
                span = (i + 1) * DH
                scores = dot(qp[h, i * DH : span, :], kT[h, :, 0:span])
                here = column[i * DH : span]
                parts = []
                for j in range(i + 1):
                    cut = slice(j * DH, (j + 1) * DH)
                    gap = here - row[:, cut]
                    if j == i:
                        gap = jnp.where(causal, gap, -jnp.inf)
                    parts.append((scores[:, cut] * jnp.exp(gap)).astype(BF16))
                masked = jnp.concatenate(parts, axis=1) if i else parts[0]
                intra[h, i * DH : span, :] = dot(masked, vh[h, 0:span, :])

    copies["q"].wait()
    spread(qb, qf, 0)
    spread(qb, qf, half)
    block_attention(*FILL[0])

    for g in range(2):
        for i in range(1, X):
            x_copy[g, i].wait_recv()

        def row_total(g, part, tile):
            total, length = None, None
            for i in range(X):
                step = xbuf[tile, i, QUARTER : QUARTER + 8, :]
                rows = xbuf[g, i, part, :]
                total = rows if total is None else scaled(step, total) + rows
                length = step if length is None else length * step
            return total, length

        total, length = row_total(g, slice(0, QUARTER), g)
        for i in range(Z):
            rbuf[g, i, 0:ZR, :] = total[i * ZR : (i + 1) * ZR]
            rbuf[g, i, ZR : ZR + 8, :] = length
        if g:
            total, _ = row_total(g, slice(QUARTER + 8, X_ROWS), ci)
            for i in range(Z):
                rbuf[g, i, ZR + 8 : ZR + 16, :] = total
        rows = pl.ds(0, ZR + 16 if g else ZR + 8)
        for i in range(1, Z):
            there = lax.rem(zi + i, Z)
            z_copy[g, i] = send(
                rbuf.at[g, there, rows], zbuf.at[g, zi, rows], z_s.at[g, i], z_r.at[g, i], {"seq_0": there}
            )
        zbuf[g, zi, rows, :] = rbuf[g, zi, rows, :]

    for name in ("dk", "dv", "dd", "si"):
        copies[name].wait()
    dkf[...] = dkb[...].astype(F32).reshape(DECODE * HEADS, DH)
    dvf[...] = dvb[...].astype(F32).reshape(DECODE * HEADS, DH)
    steps = lax.broadcasted_iota(jnp.int32, (DECODE, HEADS), 0)
    lanes = lax.broadcasted_iota(jnp.int32, (DECODE, HEADS), 1)
    run = jnp.zeros((DECODE, HEADS), F32)
    for u in range(DECODE):
        run = run + jnp.where(steps >= u, ddb[u : u + 1, :], 0.0)
    step_of = lax.broadcasted_iota(jnp.int32, (DECODE, 1), 0)
    for j in range(4):
        h = ci * 4 + j
        run_h = jnp.sum(jnp.where(lanes == h, run, 0.0), axis=1, keepdims=True)
        dq_h = dqf[pl.ds(h, DECODE, stride=HEADS), :]
        dk_h = dkf[pl.ds(h, DECODE, stride=HEADS), :]
        dv_h = dvf[pl.ds(h, DECODE, stride=HEADS), :]
        total = jnp.zeros((DECODE, DH), F32)
        for s in range(DECODE):
            score = jnp.sum(dq_h * dk_h[s : s + 1, :], axis=1, keepdims=True)
            gap = jnp.where(step_of >= s, run_h - run_h[s : s + 1, :], -jnp.inf)
            total = total + (score * jnp.exp(gap)) * dv_h[s : s + 1, :]
        dint[pl.ds(j, DECODE, stride=4), :] = total
        dexp[pl.ds(j, DECODE, stride=4), :] = jnp.broadcast_to(jnp.exp(run_h), (DECODE, DH))
        high, low = halves(si[pl.ds(h, DH, stride=HEADS), :])
        left = jnp.concatenate([dq_h, no_rows], axis=0).astype(BF16)
        rin[pl.ds(j, DECODE, stride=4), :] = (dot(left, high) + dot(left, low))[:DECODE]
    index = (zi * X + xi) * C + ci
    prior = si[pl.ds(pl.multiple_of(index * R * HEADS, 8), R * HEADS), :]
    for g in range(2):
        for r in range(R):
            sitile[g, 4 * r : 4 * r + 4, :] = prior[r * HEADS + 4 * g : r * HEADS + 4 * g + 4]

    block_attention(*FILL[1])

    for g in range(2):
        for i in range(1, Z):
            z_copy[g, i].wait_recv()
        state = sitile[g]
        for i in range(Z):
            zs[g, i] = state
            state = scaled(zbuf[g, i, ZR : ZR + 8, :], state) + zbuf[g, i, 0:ZR, :]
        for i in range(1, Z):
            there = lax.rem(zi + i, Z)
            zr_copy[g, i] = send(zs.at[g, there], zr.at[g, zi], zr_s.at[g, i], zr_r.at[g, i], {"seq_0": there})
        zr[g, zi] = zs[g, zi]
        for r in range(R):
            fs_ref[r, 4 * g : 4 * g + 4, :] = state[4 * r : 4 * r + 4]

    mine = pl.ds(pl.multiple_of(xi * 8, 8), 8)
    reading = rin[mine, :]
    for i in range(Z):
        reading = zbuf[ci, i, ZR : ZR + 8, :] * reading + zbuf[1, i, ZR + 8 : ZR + 16, :]
    reading = dexp[mine, :] * reading + dint[mine, :]
    reading = reading * lax.rsqrt(jnp.mean(reading * reading, axis=-1, keepdims=True) + norm_eps)
    for i in range(X):
        xs[1, i, QUARTER : QUARTER + 8, :] = reading

    block_attention(*FILL[2])

    for g in range(2):
        for i in range(1, Z):
            zr_copy[g, i].wait_recv()
        state = zr[g].reshape(QUARTER, DH)
        for i in range(X):
            xs[g, i, 0:QUARTER, :] = state
            if i < X - 1:
                state = scaled(xbuf[g, i, QUARTER : QUARTER + 8, :], state) + xbuf[g, i, 0:QUARTER, :]
        rows = pl.ds(0, QUARTER + 8 if g else QUARTER)
        for i in range(1, X):
            there = lax.rem(xi + i, X)
            xr_copy[g, i] = send(
                xs.at[g, there, rows], pc.at[g, xi, rows], xr_s.at[g, i], xr_r.at[g, i], {"seq_1": there}
            )
        pc[g, xi, rows, :] = xs[g, xi, rows, :]

    for g in range(2):
        for i in range(1, X):
            xr_copy[g, i].wait_recv()
        zero_decay = jnp.where(first, bbuf[g, ci, DECAY : DECAY + 8, :], cbuf[g, DECAY : DECAY + 8, :])
        for i in range(X):
            rows = slice(i * QUARTER, (i + 1) * QUARTER)
            chip = pc[g, i, 0:QUARTER, :]
            zero = jnp.where(first, bbuf[g, ci, rows, :], cbuf[g, rows, :])
            second = scaled(zero_decay, chip) + zero
            ps[g, rows, :] = jnp.where(first, second, chip)
            pp[g, ci, rows, :] = jnp.where(first, chip, second)
            if g:
                rows = slice(HALF + 8 * i, HALF + 8 * i + 8)
                ps[g, rows, :] = pc[g, i, QUARTER : QUARTER + 8, :]
                pp[g, ci, rows, :] = pc[g, i, QUARTER : QUARTER + 8, :]
        rows = pl.ds(0, HALF + 32 if g else HALF)
        cr_copy[g] = send(ps.at[g, rows], pp.at[g, ci, rows], cr_s.at[g], cr_r.at[g], {"seq_2": 1 - ci})

    outs = []
    for g in range(2):
        cr_copy[g].wait_recv()
        for j in range(4):
            h = 4 * g + j
            state = jnp.concatenate([pp.at[g, c][pl.ds(j, DH // 2, stride=4), :] for c in range(C)], axis=0)
            high, low = halves(state)
            for i in range(2):
                rows = slice(i * half, (i + 1) * half)
                queries = qp[h, rows, :]
                inter = dot(queries, high) + dot(queries, low)
                mixed = intra[h, rows, :] + ecol[h, rows, :] * inter
                mixed = mixed * lax.rsqrt(jnp.mean(mixed * mixed, axis=-1, keepdims=True) + norm_eps)
                ob[h, rows, :] = mixed.astype(BF16)
            outs.append(pltpu.make_async_copy(ob.at[h], out_hbm.at[h], out_sem.at[h]))
            outs[-1].start()
    for c in range(C):
        for i in range(X):
            for t in range(2):
                start = HALF + 8 * i + 4 * t
                dec_ref[2 * i + t, 4 * c : 4 * c + 4, :] = pp[1, c, start : start + 4, :]
    for copy in pending:
        copy.wait_send()
    for copy in outs:
        copy.wait()


def local(Z, q, k, v, log_decay, state_in, dq, dk, dv, dd):
    ZR = QUARTER // Z
    any_ref = pl.BlockSpec(memory_space=pl.ANY)
    vmem = pl.BlockSpec(memory_space=pltpu.VMEM)
    rows = (GROUP, HEADS, DH)
    flat = (GROUP * HEADS, DH)
    few = (DECODE, HEADS, DH)
    per_head = (HEADS, GROUP, DH)
    V, D = pltpu.VMEM, pltpu.SemaphoreType.DMA
    attended, final_rows, decode_out = pl.pallas_call(
        functools.partial(kernel, Z),
        name="scan_attention",
        out_shape=(
            jax.ShapeDtypeStruct(per_head, BF16),
            jax.ShapeDtypeStruct((ZR // 4, HEADS, DH), F32),
            jax.ShapeDtypeStruct(few, F32),
        ),
        in_specs=[any_ref] * 9,
        out_specs=(any_ref, vmem, vmem),
        scratch_shapes=[
            V(rows, BF16), V(rows, BF16), V(rows, BF16),
            V(flat, F32), V(flat, F32), V(flat, F32),
            V((HEADS, GROUP), F32), V((DH * HEADS, DH), F32),
            V(few, BF16), V(few, BF16), V(few, BF16), V((DECODE, HEADS), F32),
            V((DECODE * HEADS, DH), F32), V((DECODE * HEADS, DH), F32), V((DECODE * HEADS, DH), F32),
            V((DH, DH), BF16), V((HEADS, GROUP), F32), V((HEADS, GROUP), F32),
            V((HEADS, DH, GROUP), BF16), V(per_head, BF16), V(per_head, BF16),
            V(per_head, F32), V(per_head, F32), V(per_head, BF16),
            V((2, C, CORE_ROWS, DH), F32), V((2, CORE_ROWS, DH), F32),
            V((2, X, X_ROWS, DH), F32), V((2, X, X_ROWS, DH), F32),
            V((2, Z, ZR + 16, DH), F32), V((2, Z, ZR + 16, DH), F32),
            V((2, Z, ZR, DH), F32), V((2, Z, ZR, DH), F32),
            V((2, X, QUARTER + 8, DH), F32), V((2, X, QUARTER + 8, DH), F32),
            V((2, HALF + 32, DH), F32), V((2, C, HALF + 32, DH), F32),
            V((2, ZR, DH), F32), V((32, DH), F32), V((32, DH), F32), V((32, DH), F32),
            D((11,)), D((HEADS,)),
            D((2,)), D((2,)), D((2, X)), D((2, X)), D((2, Z)), D((2, Z)),
            D((2, Z)), D((2, Z)), D((2, X)), D((2, X)), D((2,)), D((2,)),
        ],
        compiler_params=pltpu.CompilerParams(collective_id=0, has_side_effects=True),
    )(q, k, v, log_decay.T, state_in.reshape(DH * HEADS, DH), dq, dk, dv, dd)
    return jnp.transpose(attended, (1, 0, 2)), final_rows, decode_out


def solution(mesh):
    heads = mesh.shape["head"]
    z = mesh.shape["seq"] // (X * C)
    split = Mesh(mesh.devices.reshape(z, X, C, heads), (*SEQ, "head"))
    return jax.shard_map(
        functools.partial(local, z),
        mesh=split,
        in_specs=(
            P(SEQ, "head", None),
            P(SEQ, "head", None),
            P(SEQ, "head", None),
            P(SEQ, "head"),
            P(None, "head", None),
            P(None, "head", None),
            P(None, "head", None),
            P(None, "head", None),
            P(None, "head"),
        ),
        out_specs=(P(SEQ, "head", None), P(SEQ, "head", None), P(None, "head", None)),
        check_vma=False,
    )
```

```python
import functools

import jax
import jax.numpy as jnp
from jax import lax
from jax.experimental import pallas as pl
from jax.experimental.pallas import tpu as pltpu
from jax.sharding import Mesh
from jax.sharding import PartitionSpec as P

GROUP = 512
DECODE = 8
DH = 128
HEADS = 8
X, C = 4, 2
SEQ = ("seq_0", "seq_1", "seq_2")
MESH = pl.DeviceIdType.MESH
F32, BF16 = jnp.float32, jnp.bfloat16
norm_eps = 1e-06

HALF = 256
QUARTER = 64
DECAY = HALF
EXTRA = HALF + 8
CORE_ROWS = HALF + 8 + 32
X_ROWS = QUARTER + 16

FILL = ((0, 2), (2, 5), (5, 8))


def halves(wide):
    high = wide.astype(BF16)
    return high, (wide - high.astype(F32)).astype(BF16)


def dot(a, b):
    return jnp.dot(a, b, preferred_element_type=F32)


def dot_nt(a, b):
    return lax.dot_general(a, b, (((1,), (1,)), ((), ())), preferred_element_type=F32)


def scaled(tile, rows):
    count = rows.shape[0]
    return (rows.reshape(count // 8, 8, DH) * tile[None]).reshape(count, DH)


def kernel(
    Z,
    q_hbm, k_hbm, v_hbm, ld_hbm, si_hbm, dq_hbm, dk_hbm, dv_hbm, dd_hbm,
    intra, ecol, qp, pp, fs_ref, dall,
    kb, vb, qb, kf, vf, qf, ldb, si, dqb, dkb, dvb, ddb, dqf, dkf, dvf,
    perm_s, cum_s, w_s, kT, vh,
    bbuf, cbuf, tbuf, xbuf, rbuf, zbuf, zs, zr, xs, pc, ps,
    sitile, base, after, rin, dint, dexp, dread, dx,
    ready, in_sem,
    core_s, core_r, x_s, x_r, z_s, z_r, zr_s, zr_r, xr_s, xr_r, cr_s, cr_r, d_s, d_r, dc_s, dc_r,
):
    ZR = QUARTER // Z
    R = ZR // 4
    ZH = Z // 2
    PAIR = 2 * ZR
    zi, xi, ci = (lax.axis_index(a) for a in SEQ)
    first = ci == 0
    place = lax.rem(zi, ZH)
    line = zi - place
    upper_half = zi >= ZH

    half = GROUP // 2
    copies = {}

    def fetch(name, src, dst, slot):
        copies[name] = pltpu.make_async_copy(src, dst, in_sem.at[slot])
        copies[name].start()

    fetch("ld", ld_hbm, ldb, 0)
    for i in range(2):
        rows = pl.ds(i * half, half)
        fetch(f"k{i}", k_hbm.at[rows], kb.at[rows], 1 + i)
    for i in range(2):
        rows = pl.ds(i * half, half)
        fetch(f"v{i}", v_hbm.at[rows], vb.at[rows], 3 + i)
    fetch("dq", dq_hbm, dqb, 5)
    fetch("q", q_hbm, qb, 6)
    fetch("dk", dk_hbm, dkb, 7)
    fetch("dv", dv_hbm, dvb, 8)
    fetch("dd", dd_hbm, ddb, 9)
    fetch("si", si_hbm, si, 10)

    barrier = pltpu.get_barrier_semaphore()
    partners = [{"seq_2": 1 - ci}]
    partners += [{"seq_1": lax.rem(xi + i, X)} for i in range(1, X)]
    for partner in partners:
        pl.semaphore_signal(barrier, inc=1, device_id=partner, device_id_type=MESH)
    for i in range(1, Z):

        @pl.when(zi + i < Z)
        def _():
            pl.semaphore_signal(barrier, inc=1, device_id={"seq_0": zi + i}, device_id_type=MESH)

    at = lax.broadcasted_iota(jnp.int32, (DH, DH), 0)
    feature = lax.broadcasted_iota(jnp.int32, (DH, DH), 1)
    r_at = at & (R - 1)
    z_at = ((at // R) & 1) * ZH + ((at // (2 * R)) & (ZH - 1))
    x_at = (at // (R * Z)) & (X - 1)
    c_at = at // (R * Z * X)
    owner_feature = ((z_at * X + x_at) * C + c_at) * R + r_at
    perm_s[...] = jnp.where(owner_feature == feature, 1.0, 0.0).astype(BF16)

    upper = jnp.where(at <= feature, 1.0, 0.0).astype(BF16)
    copies["ld"].wait()
    quarters = jnp.concatenate([ldb[:, i * DH : (i + 1) * DH] for i in range(4)], axis=0)
    p1, rest = quarters.astype(BF16), None
    rest = quarters - p1.astype(F32)
    p2 = rest.astype(BF16)
    p3 = (rest - p2.astype(F32)).astype(BF16)
    part = dot(p1, upper) + dot(p2, upper) + dot(p3, upper)
    before = jnp.zeros((HEADS, 1), F32)
    for i in range(4):
        piece = part[i * HEADS : (i + 1) * HEADS]
        cum_s[:, i * DH : (i + 1) * DH] = piece + before
        before = before + piece[:, DH - 1 : DH]
    w_s[...] = jnp.exp(before - cum_s[...])
    decay = jnp.broadcast_to(jnp.exp(before), (HEADS, DH))
    for g in range(2):
        for c in range(C):
            for i in range(2):
                bbuf[g, c, DECAY + 4 * i : DECAY + 4 * i + 4, :] = decay[4 * g : 4 * g + 4]

    pl.semaphore_wait(barrier, len(partners) + zi)
    for i in range(1, Z):

        @pl.when(zi >= i)
        def _():
            pl.semaphore_signal(ready.at[zi], inc=1, device_id={"seq_0": zi - i}, device_id_type=MESH)

    def spread(src, dst, start):
        @pl.loop(0, 4)
        def _(i):
            rows = src[pl.ds(start + i * 64, 64)].astype(F32)
            dst[pl.ds((start + i * 64) * HEADS, 64 * HEADS), :] = rows.reshape(64 * HEADS, DH)

    for i in range(2):
        copies[f"k{i}"].wait()
        spread(kb, kf, i * half)
    for i in range(2):
        copies[f"v{i}"].wait()
        spread(vb, vf, i * half)
    copies["dq"].wait()
    dqf[...] = dqb[...].astype(F32).reshape(DECODE * HEADS, DH)

    pending = []

    def send(src, dst, send_sem, recv_sem, where):
        copy = pltpu.make_async_remote_copy(
            src_ref=src, dst_ref=dst, send_sem=send_sem, recv_sem=recv_sem,
            device_id=where, device_id_type=MESH,
        )
        copy.start()
        pending.append(copy)
        return copy

    perm = perm_s[...]
    no_rows = jnp.zeros((8, DH), F32)
    core_copy, x_copy, z_copy, zr_copy, xr_copy, cr_copy = ({} for _ in range(6))
    for g in range(2):
        for j in range(4):
            h = 4 * g + j
            k_h = kf[pl.ds(h, GROUP, stride=HEADS), :].astype(BF16)
            v_h = vf[pl.ds(h, GROUP, stride=HEADS), :].astype(BF16)
            vh[h] = v_h
            dq_h = dqf[pl.ds(h, DECODE, stride=HEADS), :]
            left = jnp.concatenate([perm, jnp.concatenate([dq_h, no_rows], axis=0).astype(BF16)], axis=0)
            k_t = dot_nt(left, k_h)
            kT[h] = k_t[:DH].astype(BF16)
            high, low = halves(k_t * w_s[h : h + 1, :])
            state = dot(high, v_h) + dot(low, v_h)
            for c in range(C):
                bbuf.at[g, c][pl.ds(j, DH // 2, stride=4), :] = state[c * 64 : c * 64 + 64]
            bbuf.at[1, g][pl.ds(EXTRA + j, DECODE, stride=4), :] = state[DH : DH + DECODE]
        rows = pl.ds(0, CORE_ROWS if g else EXTRA)
        core_copy[g] = send(
            bbuf.at[g, 1 - ci, rows], cbuf.at[g, rows], core_s.at[g], core_r.at[g], {"seq_2": 1 - ci}
        )

    def core_weights(g):
        own, other = bbuf[g, ci, DECAY : DECAY + 8, :], cbuf[g, DECAY : DECAY + 8, :]
        return jnp.where(first, other, 1.0), jnp.where(first, 1.0, own), own * other

    for g in range(2):
        core_copy[g].wait_recv()
        w_own, w_other, both = core_weights(g)
        for i in range(X):
            rows = slice(i * QUARTER, (i + 1) * QUARTER)
            tbuf[g, i, 0:QUARTER, :] = scaled(w_own, bbuf[g, ci, rows, :]) + scaled(w_other, cbuf[g, rows, :])
            tbuf[g, i, QUARTER : QUARTER + 8, :] = both
        if g:
            w_own, w_other, _ = core_weights(ci)
            for i in range(X):
                rows = slice(EXTRA + 8 * i, EXTRA + 8 * i + 8)
                tbuf[g, i, QUARTER + 8 : X_ROWS, :] = w_own * bbuf[g, ci, rows, :] + w_other * cbuf[g, rows, :]
        rows = pl.ds(0, X_ROWS if g else QUARTER + 8)
        for i in range(1, X):
            there = lax.rem(xi + i, X)
            x_copy[g, i] = send(
                tbuf.at[g, there, rows], xbuf.at[g, xi, rows], x_s.at[g, i], x_r.at[g, i], {"seq_1": there}
            )
        xbuf[g, xi, rows, :] = tbuf[g, xi, rows, :]

    causal = lax.broadcasted_iota(jnp.int32, (DH, DH), 0) >= lax.broadcasted_iota(jnp.int32, (DH, DH), 1)

    def block_attention(start, stop):
        @pl.loop(start, stop)
        def _(h):
            q_h = qf[pl.ds(h, GROUP, stride=HEADS), :].astype(BF16)
            qp[h] = dot_nt(q_h, perm_s[...]).astype(BF16)
            row = cum_s[pl.ds(h, 1), :]
            column = jnp.broadcast_to(row, (DH, GROUP)).T
            ecol[h] = jnp.exp(column)
            for i in range(4):
                span = (i + 1) * DH
                scores = dot(qp[h, i * DH : span, :], kT[h, :, 0:span])
                here = column[i * DH : span]
                parts = []
                for j in range(i + 1):
                    cut = slice(j * DH, (j + 1) * DH)
                    gap = here - row[:, cut]
                    if j == i:
                        gap = jnp.where(causal, gap, -jnp.inf)
                    parts.append((scores[:, cut] * jnp.exp(gap)).astype(BF16))
                masked = jnp.concatenate(parts, axis=1) if i else parts[0]
                intra[h, i * DH : span, :] = dot(masked, vh[h, 0:span, :])

    copies["q"].wait()
    spread(qb, qf, 0)
    spread(qb, qf, half)
    block_attention(*FILL[0])

    def z_rows(g):
        return pl.ds(0, PAIR + 16 if g else PAIR + 8)

    def send_total(g, slot, there, meet):
        if meet:

            @pl.when(there > zi)
            def _():
                pl.semaphore_wait(ready.at[there], 1)

        return send(
            rbuf.at[g, lax.rem(there, ZH), z_rows(g)], zbuf.at[g, zi, z_rows(g)],
            z_s.at[g, slot], z_r.at[g, slot], {"seq_0": there},
        )

    for g in range(2):
        for i in range(1, X):
            x_copy[g, i].wait_recv()

        def row_total(g, part, tile):
            total, length = None, None
            for i in range(X):
                step = xbuf[tile, i, QUARTER : QUARTER + 8, :]
                rows = xbuf[g, i, part, :]
                total = rows if total is None else scaled(step, total) + rows
                length = step if length is None else length * step
            return total, length

        total, length = row_total(g, slice(0, QUARTER), g)
        for i in range(ZH):
            rbuf[g, i, 0:PAIR, :] = total[i * PAIR : (i + 1) * PAIR]
            rbuf[g, i, PAIR : PAIR + 8, :] = length
        if g:
            total, _ = row_total(g, slice(QUARTER + 8, X_ROWS), ci)
            for i in range(ZH):
                rbuf[g, i, PAIR + 8 : PAIR + 16, :] = total
        zbuf[g, zi, z_rows(g), :] = rbuf[g, place, z_rows(g), :]
        for i in range(1, ZH):
            z_copy[g, i] = send_total(g, i, line + lax.rem(place + i, ZH), g == 0)
    for g in range(2):
        for i in range(ZH):
            z_copy[g, ZH + i] = send_total(g, ZH + i, ZH - line + lax.rem(place + i, ZH), g == 0)

    for name in ("dk", "dv", "dd", "si"):
        copies[name].wait()
    dkf[...] = dkb[...].astype(F32).reshape(DECODE * HEADS, DH)
    dvf[...] = dvb[...].astype(F32).reshape(DECODE * HEADS, DH)
    steps = lax.broadcasted_iota(jnp.int32, (DECODE, HEADS), 0)
    lanes = lax.broadcasted_iota(jnp.int32, (DECODE, HEADS), 1)
    run = jnp.zeros((DECODE, HEADS), F32)
    for u in range(DECODE):
        run = run + jnp.where(steps >= u, ddb[u : u + 1, :], 0.0)
    step_of = lax.broadcasted_iota(jnp.int32, (DECODE, 1), 0)
    for j in range(4):
        h = ci * 4 + j
        run_h = jnp.sum(jnp.where(lanes == h, run, 0.0), axis=1, keepdims=True)
        dq_h = dqf[pl.ds(h, DECODE, stride=HEADS), :]
        dk_h = dkf[pl.ds(h, DECODE, stride=HEADS), :]
        dv_h = dvf[pl.ds(h, DECODE, stride=HEADS), :]
        total = jnp.zeros((DECODE, DH), F32)
        for s in range(DECODE):
            score = jnp.sum(dq_h * dk_h[s : s + 1, :], axis=1, keepdims=True)
            gap = jnp.where(step_of >= s, run_h - run_h[s : s + 1, :], -jnp.inf)
            total = total + (score * jnp.exp(gap)) * dv_h[s : s + 1, :]
        dint[pl.ds(j, DECODE, stride=4), :] = total
        dexp[pl.ds(j, DECODE, stride=4), :] = jnp.broadcast_to(jnp.exp(run_h), (DECODE, DH))
        high, low = halves(si[pl.ds(h, DH, stride=HEADS), :])
        left = jnp.concatenate([dq_h, no_rows], axis=0).astype(BF16)
        rin[pl.ds(j, DECODE, stride=4), :] = (dot(left, high) + dot(left, low))[:DECODE]
    for t in range(2):
        index = ((place + t * ZH) * X + xi) * C + ci
        prior = si[pl.ds(pl.multiple_of(index * R * HEADS, 8), R * HEADS), :]
        for g in range(2):
            for r in range(R):
                start = t * ZR + 4 * r
                sitile[g, start : start + 4, :] = prior[r * HEADS + 4 * g : r * HEADS + 4 * g + 4]

    block_attention(*FILL[1])

    def passed(g, state, z):
        return scaled(zbuf[g, z, PAIR : PAIR + 8, :], state) + zbuf[g, z, 0:PAIR, :]

    for g in range(2):
        for i in range(1, ZH):
            z_copy[g, i].wait_recv()

        @pl.when(upper_half)
        def _():
            for i in range(ZH):
                z_copy[g, ZH + i].wait_recv()
            state = sitile[g]
            for i in range(ZH):
                state = passed(g, state, i)
            base[g] = state

        @pl.when(jnp.logical_not(upper_half))
        def _():
            base[g] = sitile[g]

        state = base[g]
        for i in range(ZH):
            zs[g, i] = state
            state = passed(g, state, line + i)
        after[g] = state
        zr[g, place] = zs[g, place]
        for i in range(1, ZH):
            there = lax.rem(place + i, ZH)
            zr_copy[g, i] = send(
                zs.at[g, there], zr.at[g, place], zr_s.at[g, i], zr_r.at[g, i], {"seq_0": line + there}
            )

    block_attention(*FILL[2])

    for g in range(2):
        for i in range(1, ZH):
            zr_copy[g, i].wait_recv()
        state = zr[g].reshape(QUARTER, DH)
        for i in range(X):
            xs[g, i] = state
            if i < X - 1:
                state = scaled(xbuf[g, i, QUARTER : QUARTER + 8, :], state) + xbuf[g, i, 0:QUARTER, :]
        for i in range(1, X):
            there = lax.rem(xi + i, X)
            xr_copy[g, i] = send(xs.at[g, there], pc.at[g, xi], xr_s.at[g, i], xr_r.at[g, i], {"seq_1": there})
        pc[g, xi] = xs[g, xi]

    @pl.when(jnp.logical_not(upper_half))
    def _():
        for g in range(2):
            for i in range(ZH):
                z_copy[g, ZH + i].wait_recv()
            state = after[g]
            for i in range(ZH, Z):
                state = passed(g, state, i)
            after[g] = state

    for g in range(2):
        state = after[g, pl.ds(pl.multiple_of((zi // ZH) * ZR, 8), ZR), :]
        for r in range(R):
            fs_ref[r, 4 * g : 4 * g + 4, :] = state[4 * r : 4 * r + 4]
    mine = pl.ds(pl.multiple_of(xi * 8, 8), 8)
    reading = rin[mine, :]
    for i in range(Z):
        reading = zbuf[ci, i, PAIR : PAIR + 8, :] * reading + zbuf[1, i, PAIR + 8 : PAIR + 16, :]
    reading = dexp[mine, :] * reading + dint[mine, :]
    reading = reading * lax.rsqrt(jnp.mean(reading * reading, axis=-1, keepdims=True) + norm_eps)
    dread[...] = reading
    dx[xi] = reading
    d_copy = [None]
    for i in range(1, X):
        there = lax.rem(xi + i, X)
        d_copy.append(send(dread, dx.at[xi], d_s.at[i], d_r.at[i], {"seq_1": there}))

    for g in range(2):
        for i in range(1, X):
            xr_copy[g, i].wait_recv()
        zero_decay = jnp.where(first, bbuf[g, ci, DECAY : DECAY + 8, :], cbuf[g, DECAY : DECAY + 8, :])
        for i in range(X):
            rows = slice(i * QUARTER, (i + 1) * QUARTER)
            chip = pc[g, i]
            zero = jnp.where(first, bbuf[g, ci, rows, :], cbuf[g, rows, :])
            second = scaled(zero_decay, chip) + zero
            ps[g, rows, :] = jnp.where(first, second, chip)
            pp[g, ci, rows, :] = jnp.where(first, chip, second)
        cr_copy[g] = send(ps.at[g], pp.at[g, ci], cr_s.at[g], cr_r.at[g], {"seq_2": 1 - ci})
    for i in range(1, X):
        d_copy[i].wait_recv()
    dall[ci] = dx[...]
    dc_copy = send(dx, dall.at[ci], dc_s, dc_r, {"seq_2": 1 - ci})

    for g in range(2):
        cr_copy[g].wait_recv()
    dc_copy.wait_recv()
    for copy in pending:
        copy.wait_send()


def finish(
    intra, ecol, qp, pp, fs, dall, out_hbm, fs_hbm, dec_hbm, high_s, low_s, flat, ob, dec, sem
):
    copies = [pltpu.make_async_copy(fs, fs_hbm, sem.at[0])]
    copies[-1].start()
    for c in range(C):
        for i in range(X):
            for t in range(2):
                dec[2 * i + t, 4 * c : 4 * c + 4, :] = dall[c, i, 4 * t : 4 * t + 4, :]
    copies.append(pltpu.make_async_copy(dec, dec_hbm, sem.at[1]))
    copies[-1].start()
    for h in range(HEADS):
        g, j = divmod(h, 4)
        state = jnp.concatenate([pp.at[g, c][pl.ds(j, DH // 2, stride=4), :] for c in range(C)], axis=0)
        high_s[h], low_s[h] = halves(state)
    for i in range(4):
        rows = slice(i * DH, (i + 1) * DH)
        for h in range(HEADS):
            queries = qp[h, rows, :]
            inter = dot(queries, high_s[h]) + dot(queries, low_s[h])
            mixed = intra[h, rows, :] + ecol[h, rows, :] * inter
            mixed = mixed * lax.rsqrt(jnp.mean(mixed * mixed, axis=-1, keepdims=True) + norm_eps)
            flat[pl.ds(i * DH * HEADS + h, DH, stride=HEADS), :] = mixed
        ob[rows] = flat[i * DH * HEADS : (i + 1) * DH * HEADS, :].reshape(DH, HEADS, DH).astype(BF16)
        copies.append(pltpu.make_async_copy(ob.at[rows], out_hbm.at[rows], sem.at[2 + i]))
        copies[-1].start()
    for copy in copies:
        copy.wait()


def local(Z, q, k, v, log_decay, state_in, dq, dk, dv, dd):
    ZR = QUARTER // Z
    ZH, PAIR = Z // 2, 2 * ZR
    any_ref = pl.BlockSpec(memory_space=pl.ANY)
    vmem = pl.BlockSpec(memory_space=pltpu.VMEM)
    rows = (GROUP, HEADS, DH)
    flat = (GROUP * HEADS, DH)
    few = (DECODE, HEADS, DH)
    per_head = (HEADS, GROUP, DH)
    V, D = pltpu.VMEM, pltpu.SemaphoreType.DMA
    args = (q, k, v, log_decay.T, state_in.reshape(DH * HEADS, DH), dq, dk, dv, dd)
    parts = pl.pallas_call(
        functools.partial(kernel, Z),
        name="scan_attention",
        out_shape=(
            V(per_head, F32), V(per_head, F32), V(per_head, BF16), V((2, C, HALF, DH), F32),
            V((ZR // 4, HEADS, DH), F32), V((C, X, 8, DH), F32),
        ),
        in_specs=[any_ref] * 9,
        out_specs=[vmem] * 6,
        scratch_shapes=[
            V(rows, BF16), V(rows, BF16), V(rows, BF16),
            V(flat, F32), V(flat, F32), V(flat, F32),
            V((HEADS, GROUP), F32), V((DH * HEADS, DH), F32),
            V(few, BF16), V(few, BF16), V(few, BF16), V((DECODE, HEADS), F32),
            V((DECODE * HEADS, DH), F32), V((DECODE * HEADS, DH), F32), V((DECODE * HEADS, DH), F32),
            V((DH, DH), BF16), V((HEADS, GROUP), F32), V((HEADS, GROUP), F32),
            V((HEADS, DH, GROUP), BF16), V(per_head, BF16),
            V((2, C, CORE_ROWS, DH), F32), V((2, CORE_ROWS, DH), F32),
            V((2, X, X_ROWS, DH), F32), V((2, X, X_ROWS, DH), F32),
            V((2, ZH, PAIR + 16, DH), F32), V((2, Z, PAIR + 16, DH), F32),
            V((2, ZH, PAIR, DH), F32), V((2, ZH, PAIR, DH), F32),
            V((2, X, QUARTER, DH), F32), V((2, X, QUARTER, DH), F32),
            V((2, HALF, DH), F32),
            V((2, PAIR, DH), F32), V((2, PAIR, DH), F32), V((2, PAIR, DH), F32),
            V((32, DH), F32), V((32, DH), F32), V((32, DH), F32),
            V((8, DH), F32), V((X, 8, DH), F32),
            pltpu.SemaphoreType.REGULAR((Z,)), D((11,)),
            D((2,)), D((2,)), D((2, X)), D((2, X)), D((2, Z)), D((2, Z)),
            D((2, ZH)), D((2, ZH)), D((2, X)), D((2, X)), D((2,)), D((2,)),
            D((X,)), D((X,)), D(()), D(()),
        ],
        compiler_params=pltpu.CompilerParams(
            collective_id=0, has_side_effects=True, vmem_limit_bytes=32 << 20
        ),
    )(*(pltpu.with_memory_space_constraint(arg, pltpu.HBM) for arg in args))
    return pl.pallas_call(
        finish,
        name="finish",
        out_shape=(
            jax.ShapeDtypeStruct(rows, BF16),
            jax.ShapeDtypeStruct((ZR // 4, HEADS, DH), F32),
            jax.ShapeDtypeStruct(few, F32),
        ),
        in_specs=[vmem] * 6,
        out_specs=[any_ref] * 3,
        scratch_shapes=[
            V((HEADS, DH, DH), BF16), V((HEADS, DH, DH), BF16), V(flat, F32), V(rows, BF16), V(few, F32), D((6,)),
        ],
        compiler_params=pltpu.CompilerParams(vmem_limit_bytes=16 << 20),
    )(*(pltpu.with_memory_space_constraint(part, pltpu.VMEM) for part in parts))


def solution(mesh):
    heads = mesh.shape["head"]
    z = mesh.shape["seq"] // (X * C)
    split = Mesh(mesh.devices.reshape(z, X, C, heads), (*SEQ, "head"))
    return jax.shard_map(
        functools.partial(local, z),
        mesh=split,
        in_specs=(
            P(SEQ, "head", None),
            P(SEQ, "head", None),
            P(SEQ, "head", None),
            P(SEQ, "head"),
            P(None, "head", None),
            P(None, "head", None),
            P(None, "head", None),
            P(None, "head", None),
            P(None, "head"),
        ),
        out_specs=(P(SEQ, "head", None), P(SEQ, "head", None), P(None, "head", None)),
        check_vma=False,
    )
```
